32 devices in a mesh: groups: 2 (over y), blk: 4 (over z), heads: 2 (over x), sub: 2 (over core).
Axes of the slice: x: 2, y: 2, z: 4, core: 2. Of those that a mesh axis runs over, the one named last changes fastest.
Arguments:
- queries: bfloat16 [8, 64, 8, 8, 128], P(('groups', 'sub'), 'blk', 'heads'), parts along dimension 0, may hold values from -30 to 30
- key_pool: bfloat16 [256, 128, 8, 128], P(('groups', 'blk', 'sub'), None, 'heads'), parts along dimension 0, may hold values from -15 to 15
- value_pool: bfloat16 [256, 128, 8, 128], P(('groups', 'blk', 'sub'), None, 'heads'), parts along dimension 0, may hold values from -6 to 6
- page_table: int32 [8, 32], P(('groups', 'sub'), 'blk'), parts along dimension 0, may hold values from 0 to 15, as said below
- cache_lengths: int32 [8], P(('groups', 'sub')), parts along dimension 0, may hold values from 1024 to 4096
- tree_sizes: int32 [8], P(('groups', 'sub')), parts along dimension 0, may hold values from 16 to 64
- ancestor_bits: int32 [8, 64, 2], P(('groups', 'sub'), 'blk'), parts along dimension 0, may hold values from -2147483648 to 2147483647, as said below
- tree_keys: bfloat16 [8, 64, 8, 128], P(('groups', 'sub'), 'blk', 'heads'), parts along dimension 0, may hold values from -17 to 17
- tree_values: bfloat16 [8, 64, 8, 128], P(('groups', 'sub'), 'blk', 'heads'), parts along dimension 0, may hold values from -6 to 6
Outputs:
- attended: bfloat16 [8, 64, 8, 8, 128], P(('groups', 'sub'), 'blk', 'heads'), parts along dimension 0
The draws below stay inside these ranges and needn't reach their ends.
There are 2 independent parts, one for each index of `groups`. The reference program is written for one: setup_inputs(seed, part) draws one part's arguments, and reference() takes and returns one part's arrays. A program takes and returns all parts, laid end to end along the dimension named above; each array names one. Nothing has to cross between parts.
Inputs may be any that keep to these rules, and one draw needn't show every extreme that they name: `page_table`: within the rows of requests s * 2 to (s + 1) * 2 - 1 and the columns b * 8 to (b + 1) * 8 - 1, the entries are a permutation of 0 to 15. `ancestor_bits`: bit k % 32 of word k // 32 of row n is 1 exactly when node k is n or an ancestor of n; every node n > 0 has one parent with a lower number; bits for k >= 64 are 0; bit 31 is the sign bit of the word.
All inputs are finite; a program needn't handle non-finite values.
Results may differ from the reference program's by a relative error of at most 0.0055.
Values may be sent and summed in bfloat16 or wider, within the bound.
A program may use at most 64 MiB of HBM per device.

```python
import math
import jax
import jax.numpy as jnp
from jax import lax

HD = 128
KVH = 8
GROUP = 8
PAGE = 128
PAGES_DEV = 8
REQ_SUB = 2
NODES = 64
WORDS = 2
CACHE_MAX = 4096
PAGES = 32
REQ = 4
POOL_DEV = 16
POOL = 128
N_BLK = 4
N_SUB = 2


def tree_parents(key):
    sub_keys = jax.random.split(jax.random.fold_in(key, 11), REQ)
    node_ids = jnp.arange(NODES, dtype=jnp.int32)

    def one_tree(sub_key):
        raw_draw = jax.random.randint(sub_key, (NODES,), 0, 1 << 20, dtype=jnp.int32)
        reach = jnp.maximum(jnp.minimum(node_ids, 3), 1)
        return jnp.where(node_ids > 0, node_ids - 1 - raw_draw % reach, -1).astype(jnp.int32)
    return jax.vmap(one_tree)(sub_keys)


def ancestry(parents):
    identity_rows = jnp.eye(NODES, dtype=jnp.int32)

    def add_node(node, table):
        parent_at = parents[node]
        inherited = jnp.where(parent_at >= 0, table[jnp.maximum(parent_at, 0)], 0)
        return table.at[node].set(jnp.bitwise_or(inherited, identity_rows[node]))
    return lax.fori_loop(0, NODES, add_node, jnp.zeros((NODES, NODES), jnp.int32))


def tree_key_floats(key):
    drawn = 4.0 * jax.random.truncated_normal(jax.random.fold_in(key, 5), -4.0, 4.0, (REQ, NODES, KVH, HD), jnp.float32)
    return drawn


def draw_tree_keys(key, part):
    return tree_key_floats(key).astype(jnp.bfloat16)


def draw_queries(key, part):
    drawn = jax.random.truncated_normal(jax.random.fold_in(key, 7), -5.0, 5.0, (REQ, NODES, KVH, GROUP, HD), jnp.float32)
    return drawn.astype(jnp.bfloat16)


def draw_ancestor_bits(key, part):
    table = jax.vmap(ancestry)(tree_parents(key))
    padded = jnp.pad(table, ((0, 0), (0, 0), (0, WORDS * 32 - NODES)))
    grouped = padded.reshape(REQ, NODES, WORDS, 32)
    shifts = jnp.arange(32, dtype=jnp.int32)
    return jnp.sum(jnp.left_shift(grouped, shifts), axis=-1, dtype=jnp.int32)


def draw_page_table(key, part):
    sub_keys = jax.random.split(jax.random.fold_in(key, 3), N_SUB * N_BLK)
    permuted = jax.vmap(lambda sub_key: jax.random.permutation(sub_key, jnp.arange(POOL_DEV, dtype=jnp.int32)))(sub_keys)
    permuted = permuted.reshape(N_SUB, N_BLK, REQ_SUB, PAGES_DEV).transpose(0, 2, 1, 3)
    return permuted.reshape(REQ, PAGES).astype(jnp.int32)


def touch_ends(values, rng, least, top_value):
    dims = values.shape
    place = [jax.random.randint(jax.random.fold_in(rng, axis), (), 0, dims[axis]) for axis in range(len(dims))]
    values = values.at[tuple(place)].set(least)
    longest = dims.index(max(dims))
    place[longest] = (place[longest] + 1) % dims[longest]
    return values.at[tuple(place)].set(top_value)


def levels(own_key, extent, pieces, least, high):
    def one(dim, shards_of):
        steps = jax.random.uniform(jax.random.fold_in(jax.random.fold_in(own_key, 6), dim), (shards_of,), jnp.float32, least / len(pieces), high / len(pieces))
        return jnp.repeat(jnp.exp(steps), extent[dim] // shards_of).reshape((-1,) + (1,) * (len(extent) - dim - 1))

    level = one(*pieces[0])
    for cut in pieces[1:]:
        level = level * one(*cut)
    return level


def normal_values(rng, shape, scale, most, cuts=(), kind=jnp.bfloat16):
    level = levels(rng, shape, cuts, -0.22, 0.18) if cuts else 1.0
    array = jax.random.normal(rng, shape, jnp.float32) * scale * level
    return jnp.minimum(jnp.maximum(array, -most), most).astype(kind)


def setup_inputs(seed: int = 0, part: int = 0) -> dict:
    streams_of = jax.random.split(jax.random.key(seed), 10)
    part_splits = jax.random.split(jax.random.fold_in(streams_of[9], part), 10)
    return {
        "queries": draw_queries(jax.random.fold_in(jax.random.fold_in(streams_of[9], part), 71), part),
        "key_pool": normal_values(part_splits[1], (POOL, PAGE, KVH, HD), 2.5, 15.0, ((0, 8), (2, 2))),
        "value_pool": normal_values(part_splits[2], (POOL, PAGE, KVH, HD), 1.0, 6.0, ((0, 8), (2, 2))),
        "page_table": draw_page_table(jax.random.fold_in(jax.random.fold_in(streams_of[9], part), 71), part),
        "cache_lengths": touch_ends(jax.random.randint(part_splits[4], (REQ,), CACHE_MAX // 4, CACHE_MAX + 1), jax.random.fold_in(part_splits[4], 1), CACHE_MAX // 4, CACHE_MAX).astype(jnp.int32),
        "tree_sizes": touch_ends(jax.random.randint(part_splits[5], (REQ,), NODES // 4, NODES + 1), jax.random.fold_in(part_splits[5], 1), NODES // 4, NODES).astype(jnp.int32),
        "ancestor_bits": draw_ancestor_bits(jax.random.fold_in(jax.random.fold_in(streams_of[9], part), 71), part),
        "tree_keys": draw_tree_keys(jax.random.fold_in(jax.random.fold_in(streams_of[9], part), 71), part),
        "tree_values": normal_values(part_splits[8], (REQ, NODES, KVH, HD), 1.0, 6.0, ((0, 2), (1, 4), (2, 2))),
    }


BLOCKED = -1e+30

def reference(queries, key_pool, value_pool, page_table, cache_lengths, tree_sizes, ancestor_bits, tree_keys, tree_values):
    score_scale = 1.0 / math.sqrt(HD)
    sub_of = (jnp.arange(REQ, dtype=jnp.int32) // REQ_SUB).astype(jnp.int32)
    blk_of = (jnp.arange(PAGES, dtype=jnp.int32) // PAGES_DEV).astype(jnp.int32)
    slots = ((blk_of[None, :] * N_SUB + sub_of[:, None]) * POOL_DEV + page_table).astype(jnp.int32)
    shifts = jnp.arange(32, dtype=jnp.int32)
    node_ids = jnp.arange(NODES, dtype=jnp.int32)
    positions = jnp.arange(CACHE_MAX, dtype=jnp.int32)

    def attend(flat_index):
        request = (flat_index // KVH).astype(jnp.int32)
        head_at = (flat_index % KVH).astype(jnp.int32)
        slot_rows = lax.dynamic_index_in_dim(slots, request, 0, False)
        keys_all = jnp.take(key_pool, slot_rows, axis=0).reshape(CACHE_MAX, KVH, HD)
        values_all = jnp.take(value_pool, slot_rows, axis=0).reshape(CACHE_MAX, KVH, HD)
        cache_k = lax.dynamic_index_in_dim(keys_all, head_at, 1, False)
        cache_v = lax.dynamic_index_in_dim(values_all, head_at, 1, False)
        query_req = lax.dynamic_index_in_dim(queries, request, 0, False)
        query_rows = lax.dynamic_index_in_dim(query_req, head_at, 1, False).reshape(NODES * GROUP, HD)
        tree_k = lax.dynamic_index_in_dim(lax.dynamic_index_in_dim(tree_keys, request, 0, False), head_at, 1, False)
        tree_v = lax.dynamic_index_in_dim(lax.dynamic_index_in_dim(tree_values, request, 0, False), head_at, 1, False)
        word_rows = lax.dynamic_index_in_dim(ancestor_bits, request, 0, False)
        bit_table = jnp.bitwise_and(jnp.right_shift(word_rows[:, :, None], shifts), 1)
        bit_table = bit_table.reshape(NODES, WORDS * 32)[:, :NODES]
        tree_size = lax.dynamic_index_in_dim(tree_sizes, request, 0, False)
        cache_len = lax.dynamic_index_in_dim(cache_lengths, request, 0, False)
        allowed = (bit_table > 0) & (node_ids[None, :] < tree_size)
        allowed = jnp.repeat(allowed, GROUP, axis=0)
        live_mask = positions < cache_len
        cache_s = jnp.dot(query_rows, cache_k.T, preferred_element_type=jnp.float32) * score_scale
        cache_s = jnp.where(live_mask[None, :], cache_s, BLOCKED)
        tree_s = jnp.dot(query_rows, tree_k.T, preferred_element_type=jnp.float32) * score_scale
        tree_s = jnp.where(allowed, tree_s, BLOCKED)
        row_top = jnp.maximum(lax.optimization_barrier(jnp.max(cache_s, axis=1)), lax.optimization_barrier(jnp.max(tree_s, axis=1)))
        cache_w = jnp.where(live_mask[None, :], jnp.exp(cache_s - row_top[:, None]), 0.0)
        tree_w = jnp.where(allowed, jnp.exp(tree_s - row_top[:, None]), 0.0)
        totals = lax.optimization_barrier(jnp.sum(cache_w, axis=1)) + lax.optimization_barrier(jnp.sum(tree_w, axis=1))
        weighted = jnp.dot(cache_w.astype(jnp.bfloat16), cache_v, preferred_element_type=jnp.float32)
        weighted = weighted + jnp.dot(tree_w.astype(jnp.bfloat16), tree_v, preferred_element_type=jnp.float32)
        valid = jnp.repeat(node_ids < tree_size, GROUP)
        result = jnp.where(valid[:, None], weighted / totals[:, None], 0.0).astype(jnp.bfloat16)
        return result.reshape(NODES, GROUP, HD)
    gathered = lax.map(attend, jnp.arange(REQ * KVH, dtype=jnp.int32))
    return gathered.reshape(REQ, KVH, NODES, GROUP, HD).transpose(0, 2, 1, 3, 4)
```

```python
import functools
import math

import jax
import jax.numpy as jnp
from jax import lax
from jax.experimental import pallas as pl
from jax.experimental.pallas import tpu as pltpu
from jax.sharding import PartitionSpec as P

BLOCKED = -1e30
MESH = pl.DeviceIdType.MESH


def kernel(
    n,
    dims,
    table,
    lengths,
    sizes,
    q_ref,
    bits_ref,
    keys_hbm,
    values_hbm,
    tree_k,
    tree_v,
    out_ref,
    keys,
    values,
    q_all,
    bits_all,
    part,
    stats,
    got,
    got_stats,
    send,
    send_stats,
    local_sem,
    q_send,
    q_recv,
    bits_send,
    bits_recv,
    o_send,
    o_recv,
    s_send,
    s_recv,
):
    requests, heads, rows, pages, page_len, nodes_dev, words = dims
    me = lax.axis_index("blk")
    last = n - 1
    scale = math.log2(math.e) / math.sqrt(q_ref.shape[-1])

    def dev(at):
        return {"blk": lax.rem(at + n, n)}

    barrier = pltpu.get_barrier_semaphore()
    for step in (1, n - 1):
        pl.semaphore_signal(barrier, inc=1, device_id=dev(me + step), device_id_type=MESH)
    copy_k = pltpu.make_async_copy(keys_hbm, keys, local_sem.at[0])
    copy_v = pltpu.make_async_copy(values_hbm, values, local_sem.at[1])
    copy_k.start()
    copy_v.start()
    pl.semaphore_wait(barrier, 2)

    def q_copy(own, t, r, side, to):
        return pltpu.make_async_remote_copy(
            src_ref=q_ref.at[r] if own else q_all.at[t, r],
            dst_ref=q_all.at[t, r],
            send_sem=q_send.at[side, t, r],
            recv_sem=q_recv.at[t, r],
            device_id=dev(to),
            device_id_type=MESH,
        )

    def bits_copy(own, t, side, to):
        return pltpu.make_async_remote_copy(
            src_ref=bits_ref if own else bits_all.at[t],
            dst_ref=bits_all.at[t],
            send_sem=bits_send.at[side, t],
            recv_sem=bits_recv.at[t],
            device_id=dev(to),
            device_id_type=MESH,
        )

    def o_copy(t, r, side, to):
        return pltpu.make_async_remote_copy(
            src_ref=send.at[t, r],
            dst_ref=got.at[side, t, r],
            send_sem=o_send.at[t, r],
            recv_sem=o_recv.at[side, t, r],
            device_id=dev(to),
            device_id_type=MESH,
        )

    def s_copy(t, r, side, to):
        return pltpu.make_async_remote_copy(
            src_ref=send_stats.at[t, r],
            dst_ref=got_stats.at[side, t, r],
            send_sem=s_send.at[t, r],
            recv_sem=s_recv.at[side, t, r],
            device_id=dev(to),
            device_id_type=MESH,
        )

    def towards(side):
        return me + 1 - 2 * side

    def is_end(side):
        return me == last * (1 - side)

    for side in range(2):

        @pl.when(jnp.logical_not(is_end(side)))
        def _():
            bits_copy(True, me, side, towards(side)).start()
            for r in range(requests):
                q_copy(True, me, r, side, towards(side)).start()

    def attend(t, r, load_q, load_bits):
        node_of = me * nodes_dev + lax.broadcasted_iota(jnp.int32, (nodes_dev, rows), 0)
        picked = jnp.zeros((nodes_dev, rows), jnp.int32)
        for w in range(words):
            moved = jnp.right_shift(
                jnp.broadcast_to(load_bits(r, w), (nodes_dev, rows)), jnp.bitwise_and(node_of, 31)
            )
            picked = picked + jnp.where(
                jnp.right_shift(node_of, 5) == w, jnp.bitwise_and(moved, 1), 0
            )
        allowed = jnp.logical_and(picked > 0, node_of < sizes[r])
        spots = lax.broadcasted_iota(jnp.int32, (page_len, rows), 0)
        left = lengths[r] - me * (pages * page_len)

        def one_head(h, carry):
            q = load_q(r, h)
            contract = (((1,), (1,)), ((), ()))
            tree_s = lax.dot_general(
                tree_k[r, h], q, contract, preferred_element_type=jnp.float32
            )
            tree_s = jnp.where(allowed, tree_s * scale, BLOCKED)
            top = jnp.max(tree_s, axis=0, keepdims=True)
            scores = []
            for j in range(pages):
                s = lax.dot_general(
                    keys[h, table[r, j]], q, contract, preferred_element_type=jnp.float32
                )
                s = jnp.where(spots < left - j * page_len, s * scale, BLOCKED)
                top = jnp.maximum(top, jnp.max(s, axis=0, keepdims=True))
                scores.append(s)
            w = jnp.where(allowed, jnp.exp2(tree_s - top), 0.0)
            total = jnp.sum(w, axis=0, keepdims=True)
            acc = jnp.dot(
                tree_v[r, h], w.astype(jnp.bfloat16), preferred_element_type=jnp.float32
            )
            for j in range(pages):
                w = jnp.where(
                    spots < left - j * page_len, jnp.exp2(scores[j] - top), 0.0
                )
                total = total + jnp.sum(w, axis=0, keepdims=True)
                acc = acc + jnp.dot(
                    values[h, table[r, j]],
                    w.astype(jnp.bfloat16),
                    preferred_element_type=jnp.float32,
                )
            part[t, r, h] = acc
            stats[t, r, 0, pl.ds(h, 1), :] = top
            stats[t, r, 1, pl.ds(h, 1), :] = total
            return carry

        lax.fori_loop(0, heads, one_head, 0)

    def merge(side, t, r):
        def one_head(h, carry):
            mine = stats[t, r, 0, pl.ds(h, 1), :]
            theirs = got_stats[side, t, r, 0, pl.ds(h, 1), :]
            top = jnp.maximum(mine, theirs)
            a = jnp.exp2(mine - top)
            b = jnp.exp2(theirs - top)
            stats[t, r, 0, pl.ds(h, 1), :] = top
            stats[t, r, 1, pl.ds(h, 1), :] = (
                stats[t, r, 1, pl.ds(h, 1), :] * a
                + got_stats[side, t, r, 1, pl.ds(h, 1), :] * b
            )
            part[t, r, h] = part[t, r, h] * a + got[side, t, r, h].astype(jnp.float32) * b
            return carry

        lax.fori_loop(0, heads, one_head, 0)

    def ship(side, t, r):
        send[t, r] = part[t, r].astype(jnp.bfloat16)
        send_stats[t, r] = stats[t, r]
        s_copy(t, r, side, towards(side)).start()
        o_copy(t, r, side, towards(side)).start()

    copy_k.wait()
    copy_v.wait()

    def own_request(r, carry):
        attend(
            me, r, lambda r, h: q_ref[r, h], lambda r, w: bits_ref[r, pl.ds(w, 1), :]
        )
        return carry

    lax.fori_loop(0, requests, own_request, 0)

    def arrivals(d, carry):
        def one_request(r, inner):
            for side in range(2):
                t = me - d + 2 * d * side
                real = jnp.logical_and(t >= 0, t <= last)

                @pl.when(real)
                def _():
                    @pl.when(r == 0)
                    def _():
                        bits_copy(False, t, side, towards(side)).wait_recv()

                    q_copy(False, t, r, side, towards(side)).wait_recv()

                @pl.when(jnp.logical_and(real, jnp.logical_not(is_end(side))))
                def _():
                    @pl.when(r == 0)
                    def _():
                        bits_copy(False, t, side, towards(side)).start()

                    q_copy(False, t, r, side, towards(side)).start()

            def both(side, deep):
                t = me - d + 2 * d * side

                @pl.when(jnp.logical_and(t >= 0, t <= last))
                def _():
                    attend(
                        t,
                        r,
                        lambda r, h: q_all[t, r, h],
                        lambda r, w: bits_all[t, r, pl.ds(w, 1), :],
                    )

                    @pl.when(is_end(side))
                    def _():
                        ship(1 - side, t, r)

                return deep

            lax.fori_loop(0, 2, both, 0)
            return inner

        return lax.fori_loop(0, requests, one_request, carry)

    lax.fori_loop(1, n, arrivals, 0)

    def passing(s, carry):
        def turn(k, deep):
            side = jnp.where(2 * me >= n, 1 - k, k)
            t = jnp.where(side == 0, s, last - s)
            ahead = jnp.where(side == 0, t > me, t < me)
            first = me == last * side

            @pl.when(jnp.logical_and(ahead, jnp.logical_not(first)))
            def _():
                def one_request(r, inner):
                    s_copy(t, r, side, towards(side)).wait_recv()
                    o_copy(t, r, side, towards(side)).wait_recv()
                    merge(side, t, r)
                    ship(side, t, r)
                    return inner

                lax.fori_loop(0, requests, one_request, 0)

            return deep

        return lax.fori_loop(0, 2, turn, carry)

    lax.fori_loop(1, n, passing, 0)

    for r in range(requests):
        for side in range(2):

            @pl.when(me != last * side)
            def _():
                s_copy(me, r, side, towards(side)).wait_recv()
                o_copy(me, r, side, towards(side)).wait_recv()
                merge(side, me, r)

        for h in range(heads):
            scaled = part[me, r, h] / stats[me, r, 1, pl.ds(h, 1), :]
            node_at = me * nodes_dev + lax.broadcasted_iota(
                jnp.int32, scaled.shape, 1
            ) // (rows // nodes_dev)
            scaled = jnp.where(node_at < sizes[r], scaled, 0.0)
            out_ref[r, h] = jnp.transpose(scaled).astype(jnp.bfloat16)

    def finish(t, carry):
        for side in range(2):
            sent = jnp.where(side == 0, t <= me, t >= me)

            @pl.when(jnp.logical_and(sent, jnp.logical_not(is_end(side))))
            def _():
                bits_copy(False, t, side, towards(side)).wait_send()
                for r in range(requests):
                    q_copy(False, t, r, side, towards(side)).wait_send()

        @pl.when(t != me)
        def _():
            for r in range(requests):
                s_copy(t, r, 0, me + 1).wait_send()
                o_copy(t, r, 0, me + 1).wait_send()

        return carry

    lax.fori_loop(0, n, finish, 0)


def shards(
    n,
    queries,
    key_pool,
    value_pool,
    page_table,
    cache_lengths,
    tree_sizes,
    ancestor_bits,
    tree_keys,
    tree_values,
):
    requests, nodes_dev, heads, group_size, head_dim = queries.shape
    words = ancestor_bits.shape[2]
    slots, page_len = key_pool.shape[:2]
    pages = page_table.shape[1]
    rows = nodes_dev * group_size
    q = queries.transpose(0, 2, 1, 3, 4).reshape(requests, heads, rows, head_dim)
    bits = jnp.repeat(ancestor_bits.transpose(0, 2, 1), group_size, axis=2)
    keys = key_pool.transpose(2, 0, 1, 3)
    values = value_pool.transpose(2, 0, 3, 1)
    tree_k = tree_keys.transpose(0, 2, 1, 3)
    tree_v = tree_values.transpose(0, 2, 3, 1)
    dims = (requests, heads, rows, pages, page_len, nodes_dev, words)
    smem = pl.BlockSpec(memory_space=pltpu.SMEM)
    vmem = pl.BlockSpec(memory_space=pltpu.VMEM)
    whole = pl.BlockSpec(memory_space=pl.ANY)
    tile = (head_dim, rows)
    dma = pltpu.SemaphoreType.DMA
    out = pl.pallas_call(
        functools.partial(kernel, n, dims),
        out_shape=jax.ShapeDtypeStruct((requests, heads, rows, head_dim), jnp.bfloat16),
        in_specs=[smem, smem, smem, vmem, vmem, whole, whole, vmem, vmem],
        out_specs=vmem,
        scratch_shapes=[
            pltpu.VMEM(keys.shape, jnp.bfloat16),
            pltpu.VMEM(values.shape, jnp.bfloat16),
            pltpu.VMEM((n, requests, heads, rows, head_dim), jnp.bfloat16),
            pltpu.VMEM((n, requests, words, rows), jnp.int32),
            pltpu.VMEM((n, requests, heads) + tile, jnp.float32),
            pltpu.VMEM((n, requests, 2, heads, rows), jnp.float32),
            pltpu.VMEM((2, n, requests, heads) + tile, jnp.bfloat16),
            pltpu.VMEM((2, n, requests, 2, heads, rows), jnp.float32),
            pltpu.VMEM((n, requests, heads) + tile, jnp.bfloat16),
            pltpu.VMEM((n, requests, 2, heads, rows), jnp.float32),
            dma((2,)),
            dma((2, n, requests)),
            dma((n, requests)),
            dma((2, n)),
            dma((n,)),
            dma((n, requests)),
            dma((2, n, requests)),
            dma((n, requests)),
            dma((2, n, requests)),
        ],
        compiler_params=pltpu.CompilerParams(collective_id=0, has_side_effects=True),
    )(page_table, cache_lengths, tree_sizes, q, bits, keys, values, tree_k, tree_v)
    out = out.reshape(requests, heads, nodes_dev, group_size, head_dim)
    return out.transpose(0, 2, 1, 3, 4)


def solution(mesh):
    placed = (
        P(("groups", "sub"), "blk", "heads", None, None),
        P(("groups", "blk", "sub"), None, "heads", None),
        P(("groups", "blk", "sub"), None, "heads", None),
        P(("groups", "sub"), "blk"),
        P(("groups", "sub")),
        P(("groups", "sub")),
        P(("groups", "sub"), "blk", None),
        P(("groups", "sub"), "blk", "heads", None),
        P(("groups", "sub"), "blk", "heads", None),
    )
    return jax.shard_map(
        functools.partial(shards, mesh.shape["blk"]),
        mesh=mesh,
        in_specs=placed,
        out_specs=P(("groups", "sub"), "blk", "heads", None, None),
        check_vma=False,
    )
```

```python
import functools
import math

import jax
import jax.numpy as jnp
from jax import lax
from jax.experimental import pallas as pl
from jax.experimental.pallas import tpu as pltpu
from jax.sharding import PartitionSpec as P

BLOCKED = -1e30
MESH = pl.DeviceIdType.MESH


def kernel(
    n,
    dims,
    table,
    lengths,
    sizes,
    q_ref,
    bits_ref,
    keys_hbm,
    values_hbm,
    tree_k_raw,
    tree_v_raw,
    out_ref,
    raw_keys,
    raw_values,
    keys,
    values,
    tree_k,
    tree_v,
    pick,
    q_all,
    bits_all,
    part,
    stats,
    got,
    got_stats,
    send,
    send_stats,
    local_sem,
    q_send,
    q_recv,
    bits_send,
    bits_recv,
    o_send,
    o_recv,
    s_send,
    s_recv,
):
    requests, heads, batch, rows, pages, page_len, nodes_dev, words = dims
    me = lax.axis_index("blk")
    last = n - 1
    width = q_ref.shape[-1]
    chunks = requests * heads // batch
    scale = math.log2(math.e) / math.sqrt(width)
    contract = (((1,), (1,)), ((), ()))

    def dev(at):
        return {"blk": lax.rem(at + n, n)}

    barrier = pltpu.get_barrier_semaphore()
    for step in (1, n - 1):
        pl.semaphore_signal(barrier, inc=1, device_id=dev(me + step), device_id_type=MESH)
    copy_k = pltpu.make_async_copy(keys_hbm, raw_keys, local_sem.at[0])
    copy_v = pltpu.make_async_copy(values_hbm, raw_values, local_sem.at[1])
    copy_k.start()
    copy_v.start()
    pl.semaphore_wait(barrier, 2)

    def q_copy(own, t, c, side, to):
        return pltpu.make_async_remote_copy(
            src_ref=q_ref.at[c] if own else q_all.at[t, c],
            dst_ref=q_all.at[t, c],
            send_sem=q_send.at[side, t, c],
            recv_sem=q_recv.at[t, c],
            device_id=dev(to),
            device_id_type=MESH,
        )

    def bits_copy(own, t, side, to):
        return pltpu.make_async_remote_copy(
            src_ref=bits_ref if own else bits_all.at[t],
            dst_ref=bits_all.at[t],
            send_sem=bits_send.at[side, t],
            recv_sem=bits_recv.at[t],
            device_id=dev(to),
            device_id_type=MESH,
        )

    def o_copy(t, c, side, to):
        return pltpu.make_async_remote_copy(
            src_ref=send.at[t, c],
            dst_ref=got.at[side, t, c],
            send_sem=o_send.at[t, c],
            recv_sem=o_recv.at[side, t, c],
            device_id=dev(to),
            device_id_type=MESH,
        )

    def s_copy(t, c, side, to):
        return pltpu.make_async_remote_copy(
            src_ref=send_stats.at[t, c],
            dst_ref=got_stats.at[side, t, c],
            send_sem=s_send.at[t, c],
            recv_sem=s_recv.at[side, t, c],
            device_id=dev(to),
            device_id_type=MESH,
        )

    def towards(side):
        return me + 1 - 2 * side

    def is_end(side):
        return me == last * (1 - side)

    for side in range(2):

        @pl.when(jnp.logical_not(is_end(side)))
        def _():
            bits_copy(True, me, side, towards(side)).start()
            for c in range(chunks):
                q_copy(True, me, c, side, towards(side)).start()

    def sorter(count):
        row = lax.broadcasted_iota(jnp.int32, (count * heads, count * heads), 0)
        column = lax.broadcasted_iota(jnp.int32, (count * heads, count * heads), 1)
        return (column == (row % count) * heads + row // count).astype(jnp.bfloat16)

    def unit(count):
        row = lax.broadcasted_iota(jnp.int32, (count, count), 0)
        return (row == lax.broadcasted_iota(jnp.int32, (count, count), 1)).astype(jnp.bfloat16)

    def exact(a, b, dims_of=(((1,), (0,)), ((), ()))):
        moved = lax.dot_general(a, b, dims_of, preferred_element_type=jnp.float32)
        return moved.astype(jnp.bfloat16)

    group = pick.shape[0] // heads
    pick[...] = sorter(group)
    tree_sorter = sorter(nodes_dev)
    for r in range(requests):
        by_head = exact(tree_sorter, tree_k_raw[r])
        v_by_head = exact(tree_sorter, tree_v_raw[r])
        for h in range(heads):
            span = slice(h * nodes_dev, (h + 1) * nodes_dev)
            tree_k[r * heads + h] = by_head[span]
            tree_v[r * heads + h] = exact(unit(width), v_by_head[span], contract)
    flip = unit(width)
    copy_k.wait()

    def sort_keys(slot, carry):
        for at in range(page_len // group):
            by_head = exact(
                pick[...], raw_keys[slot, at * group * heads : (at + 1) * group * heads, :]
            )
            for h in range(heads):
                keys[h, slot, at * group : (at + 1) * group, :] = by_head[
                    h * group : (h + 1) * group
                ]
        return carry

    lax.fori_loop(0, raw_keys.shape[0], sort_keys, 0)
    copy_v.wait()

    def sort_values(slot, carry):
        pieces = [
            exact(pick[...], raw_values[slot, at * group * heads : (at + 1) * group * heads, :])
            for at in range(page_len // group)
        ]
        for h in range(heads):
            of_head = jnp.concatenate(
                [piece[h * group : (h + 1) * group] for piece in pieces], axis=0
            )
            values[h, slot] = exact(flip, of_head, contract)
        return carry

    lax.fori_loop(0, raw_values.shape[0], sort_values, 0)

    def attend(t, c, load_q, load_bits):
        r = c * batch // heads
        node_of = me * nodes_dev + lax.broadcasted_iota(
            jnp.int32, (nodes_dev, nodes_dev), 0
        )
        picked = jnp.zeros((nodes_dev, nodes_dev), jnp.int32)
        for w in range(words):
            moved = jnp.right_shift(
                jnp.broadcast_to(load_bits(r, w), (nodes_dev, nodes_dev)),
                jnp.bitwise_and(node_of, 31),
            )
            picked = picked + jnp.where(
                jnp.right_shift(node_of, 5) == w, jnp.bitwise_and(moved, 1), 0
            )
        picked = jnp.where(node_of < sizes[r], picked, 0)
        spread = (
            lax.broadcasted_iota(jnp.int32, (nodes_dev, rows), 0)
            == lax.broadcasted_iota(jnp.int32, (nodes_dev, rows), 1) // (rows // nodes_dev)
        ).astype(jnp.float32)
        allowed = (
            jnp.dot(picked.astype(jnp.float32), spread, preferred_element_type=jnp.float32) > 0.5
        )
        spots = lax.broadcasted_iota(jnp.int32, (page_len, rows), 0)
        left = lengths[r] - me * (pages * page_len)
        firsts = [(c * batch + i) % heads for i in range(batch)]
        tops, all_scores = [], []
        for i in range(batch):
            q = load_q(c, i)
            tree_s = lax.dot_general(
                tree_k[c * batch + i], q, contract, preferred_element_type=jnp.float32
            )
            tree_s = jnp.where(allowed, tree_s * scale, BLOCKED)
            top = jnp.max(tree_s, axis=0, keepdims=True)
            scores = []
            for j in range(pages):
                s = lax.dot_general(
                    keys[firsts[i], table[r, j]], q, contract, preferred_element_type=jnp.float32
                )
                s = jnp.where(spots < left - j * page_len, s * scale, BLOCKED)
                top = jnp.maximum(top, jnp.max(s, axis=0, keepdims=True))
                scores.append(s)
            tops.append(top)
            all_scores.append([tree_s] + scores)
        for i in range(batch):
            top = tops[i]
            w = jnp.exp2(all_scores[i][0] - top)
            total = jnp.sum(w, axis=0, keepdims=True)
            acc = jnp.dot(
                tree_v[c * batch + i], w.astype(jnp.bfloat16), preferred_element_type=jnp.float32
            )
            for j in range(pages):
                w = jnp.exp2(all_scores[i][1 + j] - top)
                total = total + jnp.sum(w, axis=0, keepdims=True)
                acc = acc + jnp.dot(
                    values[firsts[i], table[r, j]],
                    w.astype(jnp.bfloat16),
                    preferred_element_type=jnp.float32,
                )
            part[t, c, i] = acc
            stats[t, c, 0, i : i + 1, :] = top
            stats[t, c, 1, i : i + 1, :] = total

    def merge(side, t, c):
        for i in range(batch):
            mine = stats[t, c, 0, i : i + 1, :]
            theirs = got_stats[side, t, c, 0, i : i + 1, :]
            top = jnp.maximum(mine, theirs)
            a = jnp.exp2(mine - top)
            b = jnp.exp2(theirs - top)
            stats[t, c, 0, i : i + 1, :] = top
            stats[t, c, 1, i : i + 1, :] = (
                stats[t, c, 1, i : i + 1, :] * a + got_stats[side, t, c, 1, i : i + 1, :] * b
            )
            part[t, c, i] = part[t, c, i] * a + got[side, t, c, i].astype(jnp.float32) * b

    def ship(side, t, c):
        send_stats[t, c] = stats[t, c]
        send[t, c] = part[t, c].astype(jnp.bfloat16)
        s_copy(t, c, side, towards(side)).start()
        o_copy(t, c, side, towards(side)).start()

    def arrivals(d, carry):
        def one_chunk(c, inner):
            for side in range(2):
                t = me - d + 2 * d * side
                real = jnp.logical_and(t >= 0, t <= last)

                @pl.when(real)
                def _():
                    @pl.when(c == 0)
                    def _():
                        bits_copy(False, t, side, towards(side)).wait_recv()

                    q_copy(False, t, c, side, towards(side)).wait_recv()

                @pl.when(jnp.logical_and(real, jnp.logical_not(is_end(side))))
                def _():
                    @pl.when(c == 0)
                    def _():
                        bits_copy(False, t, side, towards(side)).start()

                    q_copy(False, t, c, side, towards(side)).start()

            def both(side, deep):
                t = me - d + 2 * d * side

                @pl.when(jnp.logical_and(t >= 0, t <= last))
                def _():
                    attend(
                        t,
                        c,
                        lambda c, i: q_all[t, c, i],
                        lambda r, w: bits_all[t, r, pl.ds(w, 1), :],
                    )

                    @pl.when(is_end(side))
                    def _():
                        ship(1 - side, t, c)

                return deep

            lax.fori_loop(0, 2, both, 0)
            return inner

        return lax.fori_loop(0, chunks, one_chunk, carry)

    lax.fori_loop(1, n, arrivals, 0)

    def own_chunk(c, carry):
        attend(
            me, c, lambda c, i: q_ref[c, i], lambda r, w: bits_ref[r, pl.ds(w, 1), :]
        )
        return carry

    lax.fori_loop(0, chunks, own_chunk, 0)

    def passing(s, carry):
        def turn(k, deep):
            side = jnp.where(2 * me >= n, 1 - k, k)
            t = jnp.where(side == 0, s, last - s)
            ahead = jnp.where(side == 0, t > me, t < me)
            first = me == last * side

            @pl.when(jnp.logical_and(ahead, jnp.logical_not(first)))
            def _():
                def one_chunk(c, inner):
                    s_copy(t, c, side, towards(side)).wait_recv()
                    o_copy(t, c, side, towards(side)).wait_recv()
                    merge(side, t, c)
                    ship(side, t, c)
                    return inner

                lax.fori_loop(0, chunks, one_chunk, 0)

            return deep

        return lax.fori_loop(0, 2, turn, carry)

    lax.fori_loop(1, n, passing, 0)

    def own_result(c, carry):
        for side in range(2):

            @pl.when(me != last * side)
            def _():
                s_copy(me, c, side, towards(side)).wait_recv()
                o_copy(me, c, side, towards(side)).wait_recv()
                merge(side, me, c)

        for i in range(batch):
            scaled = part[me, c, i] / stats[me, c, 1, i : i + 1, :]
            node_at = me * nodes_dev + lax.broadcasted_iota(
                jnp.int32, scaled.shape, 1
            ) // (rows // nodes_dev)
            scaled = jnp.where(node_at < sizes[c * batch // heads], scaled, 0.0)
            out_ref[c, i] = jnp.transpose(scaled).astype(jnp.bfloat16)
        return carry

    lax.fori_loop(0, chunks, own_result, 0)

    def finish(t, carry):
        for side in range(2):
            sent = jnp.where(side == 0, t <= me, t >= me)

            @pl.when(jnp.logical_and(sent, jnp.logical_not(is_end(side))))
            def _():
                bits_copy(False, t, side, towards(side)).wait_send()
                for c in range(chunks):
                    q_copy(False, t, c, side, towards(side)).wait_send()

        @pl.when(t != me)
        def _():
            for c in range(chunks):
                s_copy(t, c, 0, me + 1).wait_send()
                o_copy(t, c, 0, me + 1).wait_send()

        return carry

    lax.fori_loop(0, n, finish, 0)


def shards(
    n,
    queries,
    key_pool,
    value_pool,
    page_table,
    cache_lengths,
    tree_sizes,
    ancestor_bits,
    tree_keys,
    tree_values,
):
    requests, nodes_dev, heads, group_size, head_dim = queries.shape
    words = ancestor_bits.shape[2]
    slots, page_len = key_pool.shape[:2]
    pages = page_table.shape[1]
    rows = nodes_dev * group_size
    batch = max(1, heads // 2)
    chunks = requests * heads // batch
    group = min(page_len, max(1, 256 // heads))
    q = queries.transpose(0, 2, 1, 3, 4).reshape(chunks, batch, rows, head_dim)
    bits = ancestor_bits.transpose(0, 2, 1)
    keys = key_pool.reshape(slots, page_len * heads, head_dim)
    values = value_pool.reshape(slots, page_len * heads, head_dim)
    tree_k = tree_keys.reshape(requests, nodes_dev * heads, head_dim)
    tree_v = tree_values.reshape(requests, nodes_dev * heads, head_dim)
    dims = (requests, heads, batch, rows, pages, page_len, nodes_dev, words)
    smem = pl.BlockSpec(memory_space=pltpu.SMEM)
    vmem = pl.BlockSpec(memory_space=pltpu.VMEM)
    whole = pl.BlockSpec(memory_space=pl.ANY)
    dma = pltpu.SemaphoreType.DMA
    narrow = jnp.bfloat16
    piece = (batch, head_dim, rows)
    note = (2, batch, rows)
    out = pl.pallas_call(
        functools.partial(kernel, n, dims),
        out_shape=jax.ShapeDtypeStruct((chunks, batch, rows, head_dim), narrow),
        in_specs=[smem, smem, smem, vmem, vmem, whole, whole, vmem, vmem],
        out_specs=vmem,
        scratch_shapes=[
            pltpu.VMEM(keys.shape, narrow),
            pltpu.VMEM(values.shape, narrow),
            pltpu.VMEM((heads, slots, page_len, head_dim), narrow),
            pltpu.VMEM((heads, slots, head_dim, page_len), narrow),
            pltpu.VMEM((requests * heads, nodes_dev, head_dim), narrow),
            pltpu.VMEM((requests * heads, head_dim, nodes_dev), narrow),
            pltpu.VMEM((group * heads, group * heads), narrow),
            pltpu.VMEM((n, chunks, batch, rows, head_dim), narrow),
            pltpu.VMEM((n, requests, words, nodes_dev), jnp.int32),
            pltpu.VMEM((n, chunks) + piece, jnp.float32),
            pltpu.VMEM((n, chunks) + note, jnp.float32),
            pltpu.VMEM((2, n, chunks) + piece, narrow),
            pltpu.VMEM((2, n, chunks) + note, jnp.float32),
            pltpu.VMEM((n, chunks) + piece, narrow),
            pltpu.VMEM((n, chunks) + note, jnp.float32),
            dma((2,)),
            dma((2, n, chunks)),
            dma((n, chunks)),
            dma((2, n)),
            dma((n,)),
            dma((n, chunks)),
            dma((2, n, chunks)),
            dma((n, chunks)),
            dma((2, n, chunks)),
        ],
        compiler_params=pltpu.CompilerParams(collective_id=0, has_side_effects=True),
    )(page_table, cache_lengths, tree_sizes, q, bits, keys, values, tree_k, tree_v)
    out = out.reshape(requests, heads, nodes_dev, group_size, head_dim)
    return out.transpose(0, 2, 1, 3, 4)


def solution(mesh):
    placed = (
        P(("groups", "sub"), "blk", "heads", None, None),
        P(("groups", "blk", "sub"), None, "heads", None),
        P(("groups", "blk", "sub"), None, "heads", None),
        P(("groups", "sub"), "blk"),
        P(("groups", "sub")),
        P(("groups", "sub")),
        P(("groups", "sub"), "blk", None),
        P(("groups", "sub"), "blk", "heads", None),
        P(("groups", "sub"), "blk", "heads", None),
    )
    return jax.shard_map(
        functools.partial(shards, mesh.shape["blk"]),
        mesh=mesh,
        in_specs=placed,
        out_specs=P(("groups", "sub"), "blk", "heads", None, None),
        check_vma=False,
    )
```
